32 devices in a mesh: grp: 4 (over x, core), row: 4 (over z), col: 2 (over y).
Axes of the slice: x: 2, y: 2, z: 4, core: 2. Of those that a mesh axis runs over, the one named last changes fastest.
Arguments:
- fields: bfloat16 [4, 4, 192, 1536], P('grp', None, 'row', 'col'), may hold values from -12 to 12
- offset: int32 [1], replicated, may hold values from 0 to 191
- level_index: int32 [4], replicated, may hold values from 0 to 3, each once
- nudge_rate: float32 [4], replicated, may hold values from 0.2 to 0.9
- driving: float32 [4, 64, 64], replicated, may hold values from -4 to 4
Outputs:
- nudged: bfloat16 [4, 4, 192, 1536], P('grp', None, 'row', 'col')
The draws below stay inside these ranges and needn't reach their ends.
Inputs may be any that keep to these rules, and one draw needn't show every extreme that they name: `offset`: the footprint covers a third of the parent rows from there on, wrapping around the periodic domain. `level_index`: each parent level is fed by exactly one child level.
All inputs are finite; a program needn't handle non-finite values.
Results may differ from the reference program's by a relative error of at most 0.0034.
Values may be sent and summed in bfloat16 or wider, within the bound.
A program may use at most 64 MiB of HBM per device.

```python
import math
import jax
import jax.numpy as jnp
from jax import lax

LEVELS = 4
TILE_COLS = 768
MAX_WAVE = 32
BASIS = 64
PARENT_ROWS = 192
PARENT_COLS = 1536
N_GRP = 4


def fourier_table_drawn(positions, cell_count, max_order):
    orders = jnp.arange(1, max_order + 1, dtype=jnp.int32)
    period = 3 * cell_count
    phase_index = positions[:, None] * orders[None, :] % period
    angles = phase_index.astype(jnp.float32) * jnp.float32(2.0 * math.pi / period)
    wave_scale = jnp.float32(math.sqrt(2.0 / cell_count))
    constant = jnp.full((positions.shape[0], 1), 1.0 / math.sqrt(cell_count), jnp.float32)
    return jnp.concatenate([constant, wave_scale * jnp.cos(angles), wave_scale * jnp.sin(angles[:, :max_order - 1])], axis=1)


def draw_fields(key, part):
    key_noise = jax.random.fold_in(key, 11)
    key_parent = jax.random.fold_in(key, 12)
    key_child = jax.random.fold_in(key, 13)
    amplitude = math.sqrt(PARENT_ROWS * PARENT_COLS) / BASIS
    row_ids = jnp.arange(PARENT_ROWS, dtype=jnp.int32)
    col_ids = jnp.arange(PARENT_COLS, dtype=jnp.int32)
    row_table = fourier_table_drawn(3 * row_ids, PARENT_ROWS, MAX_WAVE)
    col_table = fourier_table_drawn(3 * col_ids, PARENT_COLS, MAX_WAVE)
    child_row_table = fourier_table_drawn((row_ids - 1) % (3 * PARENT_ROWS), PARENT_ROWS, MAX_WAVE)
    tile_ids = col_ids // TILE_COLS
    within = col_ids % TILE_COLS
    child_col_tables = jnp.stack([fourier_table_drawn(((3 * tile_ids + slot) * TILE_COLS + within - 1) % (3 * PARENT_COLS), PARENT_COLS, MAX_WAVE) for slot in range(3)])
    shape = (N_GRP, LEVELS, PARENT_ROWS, PARENT_COLS)
    noise_part = jax.random.normal(key_noise, shape, jnp.float32)
    parent_coef = jax.random.normal(key_parent, (LEVELS, BASIS, BASIS), jnp.float32) * amplitude
    child_coef = jax.random.normal(key_child, (LEVELS, BASIS, BASIS), jnp.float32) * amplitude
    parent_cols = jnp.einsum('lnm,jm->lnj', parent_coef, col_table)
    parent_smooth = jnp.einsum('in,lnj->lij', row_table, parent_cols)
    child_cols = jnp.einsum('lnm,gjm->glnj', child_coef, child_col_tables)
    child_smooth = jnp.einsum('in,glnj->glij', child_row_table, child_cols)
    smooth_part = jnp.concatenate([child_smooth, parent_smooth[None]], axis=0)
    total = jnp.clip(smooth_part + noise_part, -12.0, 12.0)
    return total.astype(jnp.bfloat16)


def noise(own_key, shape, scale, most, held_as=jnp.bfloat16):
    return jnp.clip(scale * jax.random.normal(own_key, shape, jnp.float32), -most, most).astype(held_as)


def setup_inputs(seed: int = 0) -> dict:
    key_of = jax.random.split(jax.random.key(seed), 6)
    fields = draw_fields(jax.random.fold_in(key_of[5], 71), 0)
    offset = jax.random.randint(key_of[1], (1,), 0, PARENT_ROWS).astype(jnp.int32)
    level_index = jax.random.permutation(key_of[2], LEVELS).astype(jnp.int32)
    nudge_rate = jnp.clip(jnp.exp(jax.random.uniform(key_of[3], (LEVELS,), jnp.float32, math.log(0.2), math.log(0.9))), 0.2, 0.9)
    driving = noise(key_of[4], (LEVELS, BASIS, BASIS), 1.0, 4.0, jnp.float32)
    return {"fields": fields, "offset": offset, "level_index": level_index, "nudge_rate": nudge_rate, "driving": driving}


def fourier_table(positions, cell_count, max_order):
    orders = jnp.arange(1, max_order + 1, dtype=jnp.int32)
    period = 3 * cell_count
    phase_index = positions[:, None] * orders[None, :] % period
    angles = phase_index.astype(jnp.float32) * jnp.float32(2.0 * math.pi / period)
    wave_scale = jnp.float32(math.sqrt(2.0 / cell_count))
    constant = jnp.full((positions.shape[0], 1), 1.0 / math.sqrt(cell_count), jnp.float32)
    return jnp.concatenate([constant, wave_scale * jnp.cos(angles), wave_scale * jnp.sin(angles[:, :max_order - 1])], axis=1)

def reference(fields, offset, level_index, nudge_rate, driving):
    shift_rows = offset[0]
    level_ids = jnp.arange(LEVELS, dtype=jnp.int32)
    inverse = lax.optimization_barrier(jnp.sum(level_ids[:, None] * (level_index[:, None] == level_ids[None, :]).astype(jnp.int32), axis=0))
    row_ids = jnp.arange(PARENT_ROWS, dtype=jnp.int32)
    col_ids = jnp.arange(PARENT_COLS, dtype=jnp.int32)
    row_table = fourier_table(3 * row_ids, PARENT_ROWS, MAX_WAVE)
    col_table = fourier_table(3 * col_ids, PARENT_COLS, MAX_WAVE)
    row_half = lax.optimization_barrier(row_table.astype(jnp.bfloat16))
    row_rounded = row_half.astype(jnp.float32)
    col_rounded = col_table.astype(jnp.bfloat16)
    child_row_table = fourier_table((3 * shift_rows + row_ids - 1) % (3 * PARENT_ROWS), PARENT_ROWS, MAX_WAVE)
    tile_ids = col_ids // TILE_COLS
    within = col_ids % TILE_COLS
    child_col_tables = jnp.stack([fourier_table(((3 * tile_ids + slot) * TILE_COLS + within - 1) % (3 * PARENT_COLS), PARENT_COLS, MAX_WAVE) for slot in range(3)])
    amplitude = math.sqrt(PARENT_ROWS * PARENT_COLS) / BASIS
    strip_index = (row_ids - shift_rows) % PARENT_ROWS
    covered = strip_index < PARENT_ROWS // 3
    strip_rows = jnp.clip(strip_index, 0, PARENT_ROWS // 3 - 1)

    def one_level(parent_level):
        child_level = inverse[parent_level]
        child_slots = lax.dynamic_index_in_dim(fields[:N_GRP - 1], child_level, axis=1, keepdims=False)
        parent = lax.dynamic_index_in_dim(fields[N_GRP - 1], parent_level, axis=0, keepdims=False)
        block_sums = lax.optimization_barrier(jnp.sum(child_slots.reshape(3, PARENT_ROWS // 3, 3, PARENT_COLS // 3, 3), axis=(2, 4), dtype=jnp.float32))
        averaged = (block_sums / 9.0).astype(jnp.bfloat16)
        averaged = averaged.reshape(3, PARENT_ROWS // 3, PARENT_COLS // TILE_COLS, TILE_COLS // 3)
        averaged = jnp.transpose(averaged, (1, 2, 0, 3)).reshape(PARENT_ROWS // 3, PARENT_COLS)
        fed_tile = jnp.where(covered[:, None], averaged[strip_rows], parent)
        projected = jnp.dot(fed_tile, col_rounded, preferred_element_type=jnp.float32)
        coeffs = jnp.dot(row_rounded.T, projected, precision=lax.Precision.HIGHEST)
        deficit = amplitude * driving[parent_level] - coeffs
        rate = nudge_rate[parent_level]
        spread_cols = jnp.dot(deficit, col_table.T, precision=lax.Precision.HIGHEST)
        increment = jnp.dot(row_table, spread_cols, precision=lax.Precision.HIGHEST)
        parent_new = (fed_tile.astype(jnp.float32) + rate * increment).astype(jnp.bfloat16)
        child_spread = jnp.einsum('nm,gjm->gnj', deficit, child_col_tables, precision=lax.Precision.HIGHEST)
        child_increment = jnp.einsum('in,gnj->gij', child_row_table, child_spread, precision=lax.Precision.HIGHEST)
        child_new = (child_slots.astype(jnp.float32) + rate * child_increment).astype(jnp.bfloat16)
        return (parent_new, child_new)
    parents, children = lax.map(one_level, level_ids)
    children = jnp.take(children, level_index, axis=0)
    children = jnp.transpose(children, (1, 0, 2, 3))
    return jnp.concatenate([children, parents[None]], axis=0)
```

```python
import functools
import math

import jax
import jax.numpy as jnp
from jax import lax
from jax.experimental import pallas as pl
from jax.experimental.pallas import tpu as pltpu
from jax.sharding import PartitionSpec as P

MESH = pl.DeviceIdType.MESH
F32, BF16 = jnp.float32, jnp.bfloat16


def count(shape, axis):
    return lax.broadcasted_iota(jnp.int32, shape, axis).astype(F32)


def split(index, size):
    whole = jnp.floor((index + 0.5) * (1.0 / size))
    return whole, index - size * whole


def basis(order, position, cells, top):
    period = 3 * cells
    is_sine = order > top
    wave = 4.0 * jnp.where(is_sine, order - top, order)
    phase = wave * position - jnp.where(is_sine, float(period), 0.0)
    turn = 4.0 * period
    phase = phase - turn * jnp.floor(phase * (1.0 / turn) + 0.5)
    t = (period - jnp.abs(phase)) * (math.pi / (2.0 * period))
    t2 = t * t
    poly = 1.0 / math.factorial(13)
    for degree in (11, 9, 7, 5, 3, 1):
        sign = -1.0 if degree % 4 == 3 else 1.0
        poly = poly * t2 + sign / math.factorial(degree)
    scale = jnp.where(order == 0, 1.0 / math.sqrt(cells), math.sqrt(2.0 / cells))
    return scale * (poly * t)


def halves(value):
    high = value.astype(BF16)
    return high, (value - high.astype(F32)).astype(BF16)


def dot(a, b):
    return jnp.dot(a, b, preferred_element_type=F32)


def kernel(
    sizes, offset_ref, level_ref, rate_ref, fields_ref, driving_ref, out_ref,
    tile, average, base, sent, got, passed, crossed, whole, placed_in, row_mix, col_mix, drive,
    load_sem, s1, r1, s2, r2, s3, r3, sf, rf,
):
    groups, rows, cols = sizes
    group, row, col = lax.axis_index("grp"), lax.axis_index("row"), lax.axis_index("col")
    levels, tile_rows, tile_cols = tile.shape
    size = driving_ref.shape[1]
    top = size // 2
    full_rows, full_cols = rows * tile_rows, cols * tile_cols
    third_rows, third_cols = tile_rows // 3, tile_cols // 3
    flat = levels * tile_rows
    strip = levels * third_rows
    plane = groups * cols
    pairs = levels // 2
    chunk = pairs * size // plane
    parent = groups - 1
    is_parent = group == parent
    mine = group * cols + col

    def plane_peer(step):
        other = lax.rem(mine + step, plane)
        return other, (other // cols, row, lax.rem(other, cols))

    load = pltpu.make_async_copy(fields_ref.at[0], tile, load_sem)
    load.start()

    barrier = pltpu.get_barrier_semaphore()
    for step in range(1, plane):
        pl.semaphore_signal(barrier, 1, device_id=plane_peer(step)[1], device_id_type=MESH)
    for turn in range(1, rows):
        for other in range(groups):
            pl.semaphore_signal(
                barrier, 1, device_id=(other, lax.rem(row + turn, rows), col), device_id_type=MESH
            )

    shift = offset_ref[0].astype(F32)
    row_f, col_f, group_f = row.astype(F32), col.astype(F32), group.astype(F32)

    def lookup(index, values):
        out = jnp.where(index == 0, values[0], values[1])
        for n in range(2, levels):
            out = jnp.where(index == n, values[n], out)
        return out

    targets = [level_ref[n].astype(F32) for n in range(levels)]
    rates = [rate_ref[n] for n in range(levels)]

    load.wait()

    def store_partial(mix, projected):
        high, low = halves(projected)
        coeffs = dot(mix, high) + dot(mix, low)
        lane = count((size, 2 * size), 1)
        for pair in range(pairs):
            first = coeffs[2 * pair * size : (2 * pair + 1) * size]
            second = coeffs[(2 * pair + 1) * size : (2 * pair + 2) * size]
            both = jnp.where(lane < size, first, second)
            for n in range(size // chunk):
                sent[pair * (size // chunk) + n] = both[n * chunk : (n + 1) * chunk]

    @pl.when(jnp.logical_not(is_parent))
    def _():
        d = count((tile_cols, third_cols), 0) - 3.0 * count((tile_cols, third_cols), 1)
        pick = jnp.where((d >= 0) & (d < 3), 1.0, 0.0).astype(BF16)
        summed = dot(tile[...].reshape(flat, tile_cols), pick)
        level, i = split(count((1, flat), 1), tile_rows)
        land = lookup(level, targets) * third_rows + split(i, 3)[0]
        mix = jnp.where(count((strip, flat), 0) == land, 1.0, 0.0).astype(BF16)
        high = summed.astype(BF16)
        rest = summed - high.astype(F32)
        middle, low = halves(rest)
        total = dot(mix, high) + dot(mix, middle) + dot(mix, low)
        block = (total / 9.0).astype(BF16)
        average[...] = block
        x = (3.0 * col_f + group_f) * third_cols + count((third_cols, 2 * size), 0)
        order = split(count((1, 2 * size), 1), size)[1]
        projected = dot(block, basis(order, 3.0 * x, full_cols, top).astype(BF16))
        level_to, order_to = split(count((levels * size, 1), 0), size)
        level_from, q = split(count((1, strip), 1), third_rows)
        r = row_f * third_rows + q + shift
        table = basis(order_to, 3.0 * r, full_rows, top)
        store_partial(jnp.where(level_to == level_from, table, 0.0).astype(BF16), projected)

    @pl.when(is_parent)
    def _():
        x = col_f * tile_cols + count((tile_cols, 2 * size), 0)
        order = split(count((1, 2 * size), 1), size)[1]
        table = basis(order, 3.0 * x, full_cols, top).astype(BF16)
        projected = dot(tile[...].reshape(flat, tile_cols), table)
        level_to, order_to = split(count((levels * size, 1), 0), size)
        level_from, i = split(count((1, flat), 1), tile_rows)
        r = row_f * tile_rows + i
        s = r - shift
        s = jnp.where(s < 0, s + full_rows, s)
        table = basis(order_to, 3.0 * r, full_rows, top)
        keep = (level_to == level_from) & (s >= full_rows // 3)
        store_partial(jnp.where(keep, table, 0.0).astype(BF16), projected)

    pl.semaphore_wait(barrier, plane - 1 + (rows - 1) * groups)

    scatter = []
    for step in range(1, plane):
        other, device = plane_peer(step)
        copy = pltpu.make_async_remote_copy(
            src_ref=sent.at[other], dst_ref=got.at[step - 1], send_sem=s1.at[step - 1],
            recv_sem=r1.at[step - 1], device_id=device, device_id_type=MESH,
        )
        copy.start()
        scatter.append(copy)

    def feed(g, turn, source, target):
        return pltpu.make_async_remote_copy(
            src_ref=average,
            dst_ref=placed_in.at[source, :, pl.ds(pl.multiple_of(g * third_cols, 128), third_cols)],
            send_sem=sf.at[turn], recv_sem=rf.at[g * rows + turn],
            device_id=(parent, target, col), device_id_type=MESH,
        )

    @pl.when(jnp.logical_not(is_parent))
    def _():
        for turn in range(rows):
            feed(group, turn, row, lax.rem(row + turn, rows)).start()

    level, i = split(count((flat, 1), 0), tile_rows)
    at = jnp.where(is_parent, level, lookup(level, targets))
    pair_at, half_at = split(at, 2)
    pair, order = split(count((1, pairs * size), 1), size)
    i = i + row_f * tile_rows
    z = jnp.where(is_parent, 3.0 * i, 3.0 * shift + i - 1.0)
    table = basis(order, z, full_rows, top) * lookup(at, rates)
    row_high, row_low = halves(jnp.where(pair == pair_at, table, 0.0))
    row_mix[0] = row_high
    row_mix[1] = row_low

    j = count((1, tile_cols), 1)
    z = jnp.where(
        is_parent, 3.0 * (col_f * tile_cols + j), (3.0 * col_f + group_f) * tile_cols + j - 1.0
    )
    col_high, col_low = halves(basis(count((size, 1), 0), z, full_cols, top))
    col_mix[0] = col_high
    col_mix[1] = col_high
    col_mix[2] = col_low
    col_mix[3] = col_low
    amplitude = math.sqrt(full_rows * full_cols) / size
    for pair_n in range(pairs):
        drive[pair_n] = amplitude * jnp.concatenate(
            [driving_ref[2 * pair_n], driving_ref[2 * pair_n + 1]], axis=1
        )

    total = sent[mine]
    for step in range(1, plane):
        scatter[step - 1].wait_recv()
        total = total + got[step - 1]
    passed[...] = total
    along = []
    for turn in range(1, rows):
        copy = pltpu.make_async_remote_copy(
            src_ref=passed, dst_ref=crossed.at[turn - 1], send_sem=s2.at[turn - 1],
            recv_sem=r2.at[turn - 1], device_id=(group, lax.rem(row + turn, rows), col),
            device_id_type=MESH,
        )
        copy.start()
        along.append(copy)
    for turn in range(1, rows):
        along[turn - 1].wait_recv()
        total = total + crossed[turn - 1]
    whole[mine] = total
    gather = []
    for step in range(1, plane):
        other, device = plane_peer(step)
        copy = pltpu.make_async_remote_copy(
            src_ref=whole.at[mine], dst_ref=whole.at[mine], send_sem=s3.at[step - 1],
            recv_sem=r3.at[step - 1], device_id=device, device_id_type=MESH,
        )
        copy.start()
        gather.append(copy)

    @pl.when(is_parent)
    def _():
        for g in range(groups - 1):
            for turn in range(rows):
                feed(g, turn, lax.rem(row + rows - turn, rows), row).wait_recv()
        level_to, i = split(count((flat, 1), 0), tile_rows)
        s = row_f * tile_rows + i - shift
        s = jnp.where(s < 0, s + full_rows, s)
        source, rest = split(count((1, rows * strip), 1), strip)
        level_from, q = split(rest, third_rows)
        hit = (level_to == level_from) & (s == source * third_rows + q)
        pick = jnp.where(hit, 1.0, 0.0).astype(BF16)
        arrived = dot(pick, placed_in[...].reshape(rows * strip, tile_cols)).astype(BF16)
        own = tile[...].reshape(flat, tile_cols)
        fed = jnp.where(s < full_rows // 3, arrived.astype(F32), own.astype(F32)).astype(BF16)
        base[...] = fed

    @pl.when(jnp.logical_not(is_parent))
    def _():
        base[...] = tile[...].reshape(flat, tile_cols)

    for step in range(1, plane):
        came = lax.rem(mine + plane - step, plane)
        pltpu.make_async_remote_copy(
            src_ref=whole.at[mine], dst_ref=whole.at[came], send_sem=s3.at[step - 1],
            recv_sem=r3.at[step - 1], device_id=plane_peer(step)[1], device_id_type=MESH,
        ).wait_recv()

    coeffs = jnp.concatenate([whole[n] for n in range(plane)], axis=0)
    deficit = drive[...].reshape(pairs * size, 2 * size) - coeffs
    high, low = halves(deficit)
    spread = dot(row_mix[0], high) + dot(row_mix[0], low) + dot(row_mix[1], high)
    lane_half = split(count((1, 2 * size), 1), size)[0]
    spread = jnp.where(lane_half == half_at, spread, 0.0)
    spread = spread + pltpu.roll(spread, size, 1)
    rounded = spread.astype(BF16).astype(F32)
    parts = jnp.where(lane_half == 0, rounded, spread - rounded).astype(BF16)
    mixed = jnp.concatenate([parts, parts], axis=1)
    increment = dot(mixed, col_mix[...].reshape(4 * size, tile_cols))
    result = (base[...].astype(F32) + increment).astype(BF16)
    out_ref[...] = result.reshape(1, levels, tile_rows, tile_cols)

    for copy in scatter + along + gather:
        copy.wait_send()

    @pl.when(jnp.logical_not(is_parent))
    def _():
        for turn in range(rows):
            feed(group, turn, row, lax.rem(row + turn, rows)).wait_send()


def solution(mesh):
    groups, rows, cols = (mesh.shape[name] for name in ("grp", "row", "col"))
    plane = groups * cols

    def per_device(fields, offset, level_index, nudge_rate, driving):
        _, levels, tile_rows, tile_cols = fields.shape
        size = driving.shape[1]
        strip = levels * tile_rows // 3
        flat = levels * tile_rows
        pairs = levels // 2
        chunk = pairs * size // plane
        dma = lambda n: pltpu.SemaphoreType.DMA((n,))
        vmem = pl.BlockSpec(memory_space=pltpu.VMEM)
        smem = pl.BlockSpec(memory_space=pltpu.SMEM)
        return pl.pallas_call(
            functools.partial(kernel, (groups, rows, cols)),
            out_shape=jax.ShapeDtypeStruct(fields.shape, fields.dtype),
            in_specs=[smem, smem, smem, pl.BlockSpec(memory_space=pl.ANY), vmem],
            out_specs=vmem,
            scratch_shapes=[
                pltpu.VMEM((levels, tile_rows, tile_cols), BF16),
                pltpu.VMEM((strip, tile_cols // 3), BF16),
                pltpu.VMEM((flat, tile_cols), BF16),
                pltpu.VMEM((plane, chunk, 2 * size), F32),
                pltpu.VMEM((plane - 1, chunk, 2 * size), F32),
                pltpu.VMEM((chunk, 2 * size), F32),
                pltpu.VMEM((rows - 1, chunk, 2 * size), F32),
                pltpu.VMEM((plane, chunk, 2 * size), F32),
                pltpu.VMEM((rows, strip, tile_cols), BF16),
                pltpu.VMEM((2, flat, pairs * size), BF16),
                pltpu.VMEM((4, size, tile_cols), BF16),
                pltpu.VMEM((pairs, size, 2 * size), F32),
                pltpu.SemaphoreType.DMA,
                dma(plane - 1), dma(plane - 1), dma(rows - 1), dma(rows - 1),
                dma(plane - 1), dma(plane - 1), dma(rows), dma((groups - 1) * rows),
            ],
            compiler_params=pltpu.CompilerParams(collective_id=0, has_side_effects=True),
        )(offset, level_index, nudge_rate, fields, driving)

    placed = (P("grp", None, "row", "col"), P(), P(), P(), P())
    return jax.shard_map(
        per_device,
        mesh=mesh,
        in_specs=placed,
        out_specs=P("grp", None, "row", "col"),
        check_vma=False,
    )
```

```python
import functools
import math

import jax
import jax.numpy as jnp
from jax import lax
from jax.experimental import pallas as pl
from jax.experimental.pallas import tpu as pltpu
from jax.sharding import PartitionSpec as P

MESH = pl.DeviceIdType.MESH
F32, BF16 = jnp.float32, jnp.bfloat16


def count(shape, axis):
    return lax.broadcasted_iota(jnp.int32, shape, axis).astype(F32)


def split(index, size):
    whole = jnp.floor((index + 0.5) * (1.0 / size))
    return whole, index - size * whole


def basis(order, position, cells, top):
    period = 3 * cells
    is_sine = order > top
    wave = 4.0 * jnp.where(is_sine, order - top, order)
    phase = wave * position - jnp.where(is_sine, float(period), 0.0)
    turn = 4.0 * period
    phase = phase - turn * jnp.floor(phase * (1.0 / turn) + 0.5)
    t = (period - jnp.abs(phase)) * (math.pi / (2.0 * period))
    t2 = t * t
    poly = 1.0 / math.factorial(13)
    for degree in (11, 9, 7, 5, 3, 1):
        sign = -1.0 if degree % 4 == 3 else 1.0
        poly = poly * t2 + sign / math.factorial(degree)
    scale = jnp.where(order == 0, 1.0 / math.sqrt(cells), math.sqrt(2.0 / cells))
    return scale * (poly * t)


def halves(value):
    high = value.astype(BF16)
    return high, (value - high.astype(F32)).astype(BF16)


def dot(a, b):
    return jnp.dot(a, b, preferred_element_type=F32)


def kernel(
    sizes, offset_hbm, level_hbm, rate_hbm, fields_ref, driving_hbm, out_ref,
    offset_ref, level_ref, rate_ref, driving_ref, tile, average, base, sent, got, passed, crossed, whole, placed_in, row_mix, col_mix, drive,
    load_sem, few_sem, drive_sem, s1, r1, s2, r2, s3, r3, sf, rf,
):
    groups, rows, cols = sizes
    group, row, col = lax.axis_index("grp"), lax.axis_index("row"), lax.axis_index("col")
    levels, tile_rows, tile_cols = tile.shape
    size = driving_ref.shape[1]
    top = size // 2
    full_rows, full_cols = rows * tile_rows, cols * tile_cols
    third_rows, third_cols = tile_rows // 3, tile_cols // 3
    flat = levels * tile_rows
    strip = levels * third_rows
    plane = groups * cols
    pairs = levels // 2
    chunk = pairs * size // plane
    parent = groups - 1
    is_parent = group == parent
    mine = group * cols + col

    def plane_peer(step):
        other = lax.rem(mine + step, plane)
        return other, (other // cols, row, lax.rem(other, cols))

    load = pltpu.make_async_copy(fields_ref.at[0], tile, load_sem)
    load.start()
    few = [
        pltpu.make_async_copy(offset_hbm, offset_ref, few_sem.at[0]),
        pltpu.make_async_copy(level_hbm, level_ref, few_sem.at[1]),
        pltpu.make_async_copy(rate_hbm, rate_ref, few_sem.at[2]),
    ]
    for copy in few:
        copy.start()
    load_drive = pltpu.make_async_copy(driving_hbm, driving_ref, drive_sem)
    load_drive.start()

    barrier = pltpu.get_barrier_semaphore()
    for step in range(1, plane):
        pl.semaphore_signal(barrier, 1, device_id=plane_peer(step)[1], device_id_type=MESH)
    for turn in range(1, rows):
        for other in range(groups):
            pl.semaphore_signal(
                barrier, 1, device_id=(other, lax.rem(row + turn, rows), col), device_id_type=MESH
            )

    for copy in few:
        copy.wait()
    shift = offset_ref[0].astype(F32)
    row_f, col_f, group_f = row.astype(F32), col.astype(F32), group.astype(F32)

    def lookup(index, values):
        out = jnp.where(index == 0, values[0], values[1])
        for n in range(2, levels):
            out = jnp.where(index == n, values[n], out)
        return out

    targets = [level_ref[n].astype(F32) for n in range(levels)]
    rates = [rate_ref[n] for n in range(levels)]

    def store_partial(mix, projected):
        high, low = halves(projected)
        coeffs = dot(mix, high) + dot(mix, low)
        lane = count((size, 2 * size), 1)
        for pair in range(pairs):
            first = coeffs[2 * pair * size : (2 * pair + 1) * size]
            second = coeffs[(2 * pair + 1) * size : (2 * pair + 2) * size]
            both = jnp.where(lane < size, first, second)
            for n in range(size // chunk):
                sent[pair * (size // chunk) + n] = both[n * chunk : (n + 1) * chunk]

    @pl.when(jnp.logical_not(is_parent))
    def _():
        d = count((tile_cols, third_cols), 0) - 3.0 * count((tile_cols, third_cols), 1)
        pick = jnp.where((d >= 0) & (d < 3), 1.0, 0.0).astype(BF16)
        level, i = split(count((1, flat), 1), tile_rows)
        land = lookup(level, targets) * third_rows + split(i, 3)[0]
        mix = jnp.where(count((strip, flat), 0) == land, 1.0, 0.0).astype(BF16)
        x = (3.0 * col_f + group_f) * third_cols + count((third_cols, 2 * size), 0)
        order = split(count((1, 2 * size), 1), size)[1]
        col_table = basis(order, 3.0 * x, full_cols, top).astype(BF16)
        level_to, order_to = split(count((levels * size, 1), 0), size)
        level_from, q = split(count((1, strip), 1), third_rows)
        table = basis(order_to, 3.0 * (row_f * third_rows + q + shift), full_rows, top)
        row_table = jnp.where(level_to == level_from, table, 0.0).astype(BF16)
        load.wait()
        summed = dot(tile[...].reshape(flat, tile_cols), pick)
        high = summed.astype(BF16)
        rest = summed - high.astype(F32)
        middle, low = halves(rest)
        total = dot(mix, high) + dot(mix, middle) + dot(mix, low)
        block = (total / 9.0).astype(BF16)
        average[...] = block
        store_partial(row_table, dot(block, col_table))

    @pl.when(is_parent)
    def _():
        x = col_f * tile_cols + count((tile_cols, 2 * size), 0)
        order = split(count((1, 2 * size), 1), size)[1]
        col_table = basis(order, 3.0 * x, full_cols, top).astype(BF16)
        level_to, order_to = split(count((levels * size, 1), 0), size)
        level_from, i = split(count((1, flat), 1), tile_rows)
        r = row_f * tile_rows + i
        s = r - shift
        s = jnp.where(s < 0, s + full_rows, s)
        table = basis(order_to, 3.0 * r, full_rows, top)
        keep = (level_to == level_from) & (s >= full_rows // 3)
        row_table = jnp.where(keep, table, 0.0).astype(BF16)
        load.wait()
        store_partial(row_table, dot(tile[...].reshape(flat, tile_cols), col_table))

    pl.semaphore_wait(barrier, plane - 1 + (rows - 1) * groups)

    scatter = []
    for step in range(1, plane):
        other, device = plane_peer(step)
        copy = pltpu.make_async_remote_copy(
            src_ref=sent.at[other], dst_ref=got.at[step - 1], send_sem=s1.at[step - 1],
            recv_sem=r1.at[step - 1], device_id=device, device_id_type=MESH,
        )
        copy.start()
        scatter.append(copy)

    def feed(g, turn, source, target):
        return pltpu.make_async_remote_copy(
            src_ref=average,
            dst_ref=placed_in.at[source, :, pl.ds(pl.multiple_of(g * third_cols, 128), third_cols)],
            send_sem=sf.at[turn], recv_sem=rf.at[g * rows + turn],
            device_id=(parent, target, col), device_id_type=MESH,
        )

    level, i = split(count((flat, 1), 0), tile_rows)
    at = jnp.where(is_parent, level, lookup(level, targets))
    pair_at, half_at = split(at, 2)
    pair, order = split(count((1, pairs * size), 1), size)
    i = i + row_f * tile_rows
    z = jnp.where(is_parent, 3.0 * i, 3.0 * shift + i - 1.0)
    table = basis(order, z, full_rows, top) * lookup(at, rates)
    row_high, row_low = halves(jnp.where(pair == pair_at, table, 0.0))
    row_mix[0] = row_high
    row_mix[1] = row_low

    j = count((1, tile_cols), 1)
    z = jnp.where(
        is_parent, 3.0 * (col_f * tile_cols + j), (3.0 * col_f + group_f) * tile_cols + j - 1.0
    )
    col_high, col_low = halves(basis(count((size, 1), 0), z, full_cols, top))
    col_mix[0] = col_high
    col_mix[1] = col_high
    col_mix[2] = col_low
    col_mix[3] = col_low
    amplitude = math.sqrt(full_rows * full_cols) / size
    load_drive.wait()
    for pair_n in range(pairs):
        drive[pair_n] = amplitude * jnp.concatenate(
            [driving_ref[2 * pair_n], driving_ref[2 * pair_n + 1]], axis=1
        )

    total = sent[mine]
    for step in range(1, plane):
        scatter[step - 1].wait_recv()
        total = total + got[step - 1]
    passed[...] = total
    along = []
    for turn in range(1, rows):
        copy = pltpu.make_async_remote_copy(
            src_ref=passed, dst_ref=crossed.at[turn - 1], send_sem=s2.at[turn - 1],
            recv_sem=r2.at[turn - 1], device_id=(group, lax.rem(row + turn, rows), col),
            device_id_type=MESH,
        )
        copy.start()
        along.append(copy)
    @pl.when(jnp.logical_not(is_parent))
    def _():
        for turn in range(rows):
            feed(group, turn, row, lax.rem(row + turn, rows)).start()

    for turn in range(1, rows):
        along[turn - 1].wait_recv()
        total = total + crossed[turn - 1]
    whole[mine] = total
    gather = []
    for step in range(1, plane):
        other, device = plane_peer(step)
        copy = pltpu.make_async_remote_copy(
            src_ref=whole.at[mine], dst_ref=whole.at[mine], send_sem=s3.at[step - 1],
            recv_sem=r3.at[step - 1], device_id=device, device_id_type=MESH,
        )
        copy.start()
        gather.append(copy)

    @pl.when(is_parent)
    def _():
        for g in range(groups - 1):
            for turn in range(rows):
                feed(g, turn, lax.rem(row + rows - turn, rows), row).wait_recv()
        level_to, i = split(count((flat, 1), 0), tile_rows)
        s = row_f * tile_rows + i - shift
        s = jnp.where(s < 0, s + full_rows, s)
        source, rest = split(count((1, rows * strip), 1), strip)
        level_from, q = split(rest, third_rows)
        hit = (level_to == level_from) & (s == source * third_rows + q)
        pick = jnp.where(hit, 1.0, 0.0).astype(BF16)
        arrived = dot(pick, placed_in[...].reshape(rows * strip, tile_cols)).astype(BF16)
        own = tile[...].reshape(flat, tile_cols)
        fed = jnp.where(s < full_rows // 3, arrived.astype(F32), own.astype(F32)).astype(BF16)
        base[...] = fed

    @pl.when(jnp.logical_not(is_parent))
    def _():
        base[...] = tile[...].reshape(flat, tile_cols)

    for step in range(1, plane):
        came = lax.rem(mine + plane - step, plane)
        pltpu.make_async_remote_copy(
            src_ref=whole.at[mine], dst_ref=whole.at[came], send_sem=s3.at[step - 1],
            recv_sem=r3.at[step - 1], device_id=plane_peer(step)[1], device_id_type=MESH,
        ).wait_recv()

    coeffs = jnp.concatenate([whole[n] for n in range(plane)], axis=0)
    deficit = drive[...].reshape(pairs * size, 2 * size) - coeffs
    high, low = halves(deficit)
    spread = dot(row_mix[0], high) + dot(row_mix[0], low) + dot(row_mix[1], high)
    lane_half = split(count((1, 2 * size), 1), size)[0]
    spread = jnp.where(lane_half == half_at, spread, 0.0)
    spread = spread + pltpu.roll(spread, size, 1)
    rounded = spread.astype(BF16).astype(F32)
    parts = jnp.where(lane_half == 0, rounded, spread - rounded).astype(BF16)
    mixed = jnp.concatenate([parts, parts], axis=1)
    increment = dot(mixed, col_mix[...].reshape(4 * size, tile_cols))
    result = (base[...].astype(F32) + increment).astype(BF16)
    out_ref[...] = result.reshape(1, levels, tile_rows, tile_cols)

    for copy in scatter + along + gather:
        copy.wait_send()

    @pl.when(jnp.logical_not(is_parent))
    def _():
        for turn in range(rows):
            feed(group, turn, row, lax.rem(row + turn, rows)).wait_send()


def solution(mesh):
    groups, rows, cols = (mesh.shape[name] for name in ("grp", "row", "col"))
    plane = groups * cols

    def per_device(fields, offset, level_index, nudge_rate, driving):
        _, levels, tile_rows, tile_cols = fields.shape
        size = driving.shape[1]
        strip = levels * tile_rows // 3
        flat = levels * tile_rows
        pairs = levels // 2
        chunk = pairs * size // plane
        dma = lambda n: pltpu.SemaphoreType.DMA((n,))
        here = pl.BlockSpec(memory_space=pl.ANY)
        return pl.pallas_call(
            functools.partial(kernel, (groups, rows, cols)),
            out_shape=jax.ShapeDtypeStruct(fields.shape, fields.dtype),
            in_specs=[here] + [pl.BlockSpec(memory_space=pltpu.HBM)] * 4,
            out_specs=pl.BlockSpec(memory_space=pltpu.VMEM),
            scratch_shapes=[
                pltpu.SMEM(offset.shape, offset.dtype),
                pltpu.SMEM(level_index.shape, level_index.dtype),
                pltpu.SMEM(nudge_rate.shape, nudge_rate.dtype),
                pltpu.VMEM(driving.shape, driving.dtype),
                pltpu.VMEM((levels, tile_rows, tile_cols), BF16),
                pltpu.VMEM((strip, tile_cols // 3), BF16),
                pltpu.VMEM((flat, tile_cols), BF16),
                pltpu.VMEM((plane, chunk, 2 * size), F32),
                pltpu.VMEM((plane - 1, chunk, 2 * size), F32),
                pltpu.VMEM((chunk, 2 * size), F32),
                pltpu.VMEM((rows - 1, chunk, 2 * size), F32),
                pltpu.VMEM((plane, chunk, 2 * size), F32),
                pltpu.VMEM((rows, strip, tile_cols), BF16),
                pltpu.VMEM((2, flat, pairs * size), BF16),
                pltpu.VMEM((4, size, tile_cols), BF16),
                pltpu.VMEM((pairs, size, 2 * size), F32),
                pltpu.SemaphoreType.DMA, dma(3), pltpu.SemaphoreType.DMA,
                dma(plane - 1), dma(plane - 1), dma(rows - 1), dma(rows - 1),
                dma(plane - 1), dma(plane - 1), dma(rows), dma((groups - 1) * rows),
            ],
            compiler_params=pltpu.CompilerParams(
                collective_id=0, has_side_effects=True, vmem_limit_bytes=36 * 2**20
            ),
        )(
            offset,
            *(pltpu.with_memory_space_constraint(v, pltpu.HBM) for v in (level_index, nudge_rate, fields, driving)),
        )

    placed = (P("grp", None, "row", "col"), P(), P(), P(), P())
    return jax.shard_map(
        per_device,
        mesh=mesh,
        in_specs=placed,
        out_specs=P("grp", None, "row", "col"),
        check_vma=False,
    )
```
